128 devices in a mesh: dp: 1, cp: 128 (over z, y, x, core).
Axes of the slice: x: 4, y: 4, z: 4, core: 2. Of those that a mesh axis runs over, the one named last changes fastest.
Arguments:
- x_in: bfloat16 [2048, 5120], P(('dp', 'cp'))
- dy_in: bfloat16 [2048, 5120], P(('dp', 'cp'))
- w_q: bfloat16 [5120, 40, 128], replicated
- w_k: bfloat16 [5120, 40, 128], replicated
- w_v: bfloat16 [5120, 40, 128], replicated
- w_o: bfloat16 [40, 128, 5120], replicated
Outputs:
- output 1: bfloat16 [2048, 5120], P(('dp', 'cp'))
- output 2: bfloat16 [2048, 5120], P(('dp', 'cp'))
All inputs are finite; a program needn't handle non-finite values.
Results may differ from the reference program's by a relative error of at most 0.0107894.
Values are sent between devices in bfloat16 or wider.
A program may use at most 1 GiB of HBM per device.

```python
import jax
import jax.numpy as jnp
from jax import lax

GROUP_DEVS = 128
TOKENS_DEV = 16
MODEL_DIM = 5120
NUM_HEADS = 40
HEAD_DIM = 128


def setup_inputs(seed: int = 0, part: int = 0) -> dict:
    seq_len = GROUP_DEVS * TOKENS_DEV
    part_key = jax.random.fold_in(jax.random.key(seed), part)
    key_x, key_dy = jax.random.split(part_key)
    key_q, key_k, key_v, key_o = jax.random.split(jax.random.key(seed + 1), 4)
    in_scale = MODEL_DIM ** -0.5
    out_scale = (NUM_HEADS * HEAD_DIM) ** -0.5
    proj_shape = (MODEL_DIM, NUM_HEADS, HEAD_DIM)
    x_in = jax.random.normal(key_x, (seq_len, MODEL_DIM), jnp.float32)
    dy_in = jax.random.normal(key_dy, (seq_len, MODEL_DIM), jnp.float32)
    w_q = 2.0 * in_scale * jax.random.normal(key_q, proj_shape, jnp.float32)
    w_k = in_scale * jax.random.normal(key_k, proj_shape, jnp.float32)
    w_v = in_scale * jax.random.normal(key_v, proj_shape, jnp.float32)
    w_o = out_scale * jax.random.normal(key_o, (NUM_HEADS, HEAD_DIM, MODEL_DIM), jnp.float32)
    return {
        "x_in": x_in.astype(jnp.bfloat16),
        "dy_in": dy_in.astype(jnp.bfloat16),
        "w_q": w_q.astype(jnp.bfloat16),
        "w_k": w_k.astype(jnp.bfloat16),
        "w_v": w_v.astype(jnp.bfloat16),
        "w_o": w_o.astype(jnp.bfloat16),
    }


def layout_positions(group_devs, tok_dev):
    half_len = tok_dev // 2
    dev_ids = jnp.arange(group_devs, dtype=jnp.int32)[:, None, None]
    side_ids = jnp.arange(2, dtype=jnp.int32)[None, :, None]
    offsets = jnp.arange(half_len, dtype=jnp.int32)[None, None, :]
    piece_ids = jnp.where(side_ids == 0, dev_ids, 2 * group_devs - 1 - dev_ids)
    return (piece_ids * half_len + offsets).reshape(group_devs, tok_dev)


def reference(x_in, dy_in, w_q, w_k, w_v, w_o):
    seq_len = GROUP_DEVS * TOKENS_DEV
    score_scale = HEAD_DIM ** -0.5
    positions = layout_positions(GROUP_DEVS, TOKENS_DEV)
    key_pos = positions.reshape(seq_len)
    x_f32 = x_in.astype(jnp.float32)

    def project(weight):
        return jnp.einsum("sd,dhe->hse", x_f32, weight.astype(jnp.float32)).astype(jnp.bfloat16)

    q_heads = project(w_q)
    k_f32 = project(w_k).astype(jnp.float32)
    v_f32 = project(w_v).astype(jnp.float32)
    q_blocks = q_heads.reshape(NUM_HEADS, GROUP_DEVS, TOKENS_DEV, HEAD_DIM).transpose(1, 0, 2, 3)

    def block_probs(q_blk, q_pos):
        scores = jnp.einsum("hqe,hke->hqk", q_blk.astype(jnp.float32), k_f32) * score_scale
        causal = q_pos[:, None] >= key_pos[None, :]
        scores = jnp.where(causal[None], scores, -jnp.inf)
        log_norm = jax.nn.logsumexp(scores, axis=-1, keepdims=True)
        return jnp.exp(scores - log_norm).astype(jnp.bfloat16).astype(jnp.float32)

    def fwd_block(block_args):
        q_blk, q_pos = block_args
        attn_probs = block_probs(q_blk, q_pos)
        return jnp.einsum("hqk,hke->hqe", attn_probs, v_f32).astype(jnp.bfloat16)

    out_blocks = lax.map(fwd_block, (q_blocks, positions))
    out_rows = out_blocks.transpose(0, 2, 1, 3).reshape(seq_len, NUM_HEADS, HEAD_DIM)
    w_o_f32 = w_o.astype(jnp.float32)
    y_out = jnp.einsum("she,hed->sd", out_rows.astype(jnp.float32), w_o_f32).astype(jnp.bfloat16)
    dout_rows = jnp.einsum("sd,hed->she", dy_in.astype(jnp.float32), w_o_f32).astype(jnp.bfloat16)
    dout_blocks = dout_rows.reshape(GROUP_DEVS, TOKENS_DEV, NUM_HEADS, HEAD_DIM).transpose(0, 2, 1, 3)

    def bwd_block(acc_pair, block_args):
        dk_acc, dv_acc = acc_pair
        q_blk, q_pos, out_blk, dout_blk = block_args
        attn_probs = block_probs(q_blk, q_pos)
        dout_f32 = dout_blk.astype(jnp.float32)
        row_delta = jnp.sum(dout_f32 * out_blk.astype(jnp.float32), axis=-1, keepdims=True)
        d_probs = jnp.einsum("hqe,hke->hqk", dout_f32, v_f32)
        d_scores = (attn_probs * (d_probs - row_delta)).astype(jnp.bfloat16).astype(jnp.float32)
        d_query = (jnp.einsum("hqk,hke->hqe", d_scores, k_f32) * score_scale).astype(jnp.bfloat16)
        dk_acc = dk_acc + jnp.einsum("hqk,hqe->hke", d_scores, q_blk.astype(jnp.float32)) * score_scale
        dv_acc = dv_acc + jnp.einsum("hqk,hqe->hke", attn_probs, dout_f32)
        return (dk_acc, dv_acc), d_query

    zero_acc = jnp.zeros((NUM_HEADS, seq_len, HEAD_DIM), jnp.float32)
    (dk_total, dv_total), dq_blocks = lax.scan(
        bwd_block, (zero_acc, zero_acc), (q_blocks, positions, out_blocks, dout_blocks))
    dq_rows = dq_blocks.transpose(0, 2, 1, 3).reshape(seq_len, NUM_HEADS, HEAD_DIM)
    dk_rows = dk_total.astype(jnp.bfloat16).transpose(1, 0, 2)
    dv_rows = dv_total.astype(jnp.bfloat16).transpose(1, 0, 2)
    dx_acc = (
        jnp.einsum("she,dhe->sd", dq_rows.astype(jnp.float32), w_q.astype(jnp.float32))
        + jnp.einsum("she,dhe->sd", dk_rows.astype(jnp.float32), w_k.astype(jnp.float32))
        + jnp.einsum("she,dhe->sd", dv_rows.astype(jnp.float32), w_v.astype(jnp.float32))
    )
    return y_out, dx_acc.astype(jnp.bfloat16)
```

```python
import functools

import jax
import jax.numpy as jnp
from jax import lax
from jax.experimental import pallas as pl
from jax.experimental.pallas import tpu as pltpu
from jax.sharding import PartitionSpec as P

LOG2E = 1.4426950408889634
QB, KB = 512, 256
F32 = jnp.float32
BF16 = jnp.bfloat16


def head_home(h, heads, devs):
    return (h * (devs // 2) // heads) * 2 + 1


def home_head(me, heads, devs):
    chips = devs // 2
    chip = me // 2
    h = (chip * heads + chips - 1) // chips
    has = (me % 2 == 1) & (h < heads) & ((h * chips) // heads == chip)
    return h, has


def gather_kernel(heads, devs, src, dst, send_sem, recv_sem):
    me = lax.axis_index("cp")
    _, has = home_head(me, heads, devs)

    def send(n, carry):
        h = lax.rem(n + me, heads)
        home = head_home(h, heads, devs)
        for side in range(2):
            piece = me if side == 0 else 2 * devs - 1 - me

            @pl.when(home != me)
            def _():
                pltpu.make_async_remote_copy(
                    src_ref=src.at[h, :, side], dst_ref=dst.at[:, piece],
                    send_sem=send_sem, recv_sem=recv_sem,
                    device_id={"cp": home}, device_id_type=pl.DeviceIdType.MESH).start()

            @pl.when(home == me)
            def _():
                pltpu.make_async_copy(src.at[h, :, side], dst.at[:, piece], recv_sem).start()

        return carry

    lax.fori_loop(0, heads, send, 0)

    @pl.when(has)
    def _():
        sent = src.at[pl.ds(0, heads - 1)]
        pltpu.make_async_copy(sent, sent, send_sem).wait()
        pltpu.make_async_copy(dst, dst, recv_sem).wait()

    @pl.when(jnp.logical_not(has))
    def _():
        pltpu.make_async_copy(src, src, send_sem).wait()


def scatter_kernel(heads, devs, src, dst, send_sem, recv_sem):
    me = lax.axis_index("cp")
    mine, has = home_head(me, heads, devs)

    @pl.when(has)
    def _():
        def send(n, carry):
            to = lax.rem(n + 1 + me, devs)
            for side in range(2):
                piece = to if side == 0 else 2 * devs - 1 - to
                pltpu.make_async_remote_copy(
                    src_ref=src.at[:, piece], dst_ref=dst.at[mine, :, side],
                    send_sem=send_sem, recv_sem=recv_sem,
                    device_id={"cp": to}, device_id_type=pl.DeviceIdType.MESH).start()
            return carry

        for side in range(2):
            piece = me if side == 0 else 2 * devs - 1 - me
            pltpu.make_async_copy(src.at[:, piece], dst.at[mine, :, side], recv_sem).start()
        lax.fori_loop(0, devs - 1, send, 0)

    pltpu.make_async_copy(dst, dst, recv_sem).wait()

    @pl.when(has)
    def _():
        sent = src.at[:, pl.ds(0, 2 * devs - 2)]
        pltpu.make_async_copy(sent, sent, send_sem).wait()


def dot(a, b, dims):
    return lax.dot_general(a, b, (dims, ((), ())), preferred_element_type=F32)


NN = ((1,), (0,))
NT = ((1,), (1,))


def attend_kernel(heads, devs, qb, kb, x_ref, out_ref, kt, vt, dot_t, s_scr, p_scr, dk_acc, dv_acc, oq_scr):
    me = lax.axis_index("cp")
    _, has = home_head(me, heads, devs)
    seq, e = x_ref.shape[1], x_ref.shape[2]
    c = e ** -0.5
    k2 = c * LOG2E
    nqb = seq // qb
    per = qb // kb

    @pl.when(has)
    def _():
        def prep(i, carry):
            rows = pl.ds(pl.multiple_of(i * kb, kb), kb)
            kt[:, rows] = x_ref[1, rows, :].T
            vt[:, rows] = x_ref[2, rows, :].T
            dot_t[:, rows] = x_ref[3, rows, :].T
            dk_acc[rows, :] = jnp.zeros((kb, e), F32)
            dv_acc[rows, :] = jnp.zeros((kb, e), F32)
            return carry

        lax.fori_loop(0, seq // kb, prep, 0)

        def q_block(i, carry):
            qrows = pl.ds(pl.multiple_of(i * qb, qb), qb)
            q = x_ref[0, qrows, :]
            do = x_ref[3, qrows, :]
            full = i * per

            def krows(j):
                return pl.ds(pl.multiple_of(j * kb, kb), kb)

            def scores(j, m, masked):
                s = dot(x_ref[1, krows(j), :], q, NT)
                if masked:
                    kpos = j * kb + lax.broadcasted_iota(jnp.int32, (kb, qb), 0)
                    qpos = i * qb + lax.broadcasted_iota(jnp.int32, (kb, qb), 1)
                    s = jnp.where(qpos >= kpos, s, -jnp.inf)
                s_scr[krows(j), :] = s
                return jnp.maximum(m, jnp.max(s.reshape(kb // 8, 8, qb), axis=0))

            m8 = jnp.full((8, qb), -jnp.inf, F32)
            m8 = lax.fori_loop(0, full, lambda j, m: scores(j, m, False), m8)
            for d in range(per):
                m8 = scores(full + d, m8, True)
            m = jnp.max(m8, axis=0, keepdims=True) * k2

            def exps(j, l):
                p = jnp.exp2(s_scr[krows(j), :] * k2 - m)
                s_scr[krows(j), :] = p
                return l + jnp.sum(p.reshape(kb // 8, 8, qb), axis=0)

            l8 = lax.fori_loop(0, full + per, exps, jnp.zeros((8, qb), F32))
            inv = 1.0 / jnp.sum(l8, axis=0, keepdims=True)

            oq_scr[...] = jnp.zeros_like(oq_scr)

            def probs(j, carry):
                p = (s_scr[krows(j), :] * inv).astype(BF16)
                p_scr[krows(j), :] = p
                oq_scr[...] += dot(vt[:, krows(j)], p, NN)
                return carry

            lax.fori_loop(0, full + per, probs, 0)
            o_t = oq_scr[...].astype(BF16)
            delta = jnp.sum(o_t.astype(F32) * dot_t[:, qrows].astype(F32), axis=0, keepdims=True)
            out_ref[0, qrows, :] = o_t.T
            oq_scr[...] = jnp.zeros_like(oq_scr)

            def back(j, carry):
                p = p_scr[krows(j), :]
                dp = dot(x_ref[2, krows(j), :], do, NT)
                ds = (p.astype(F32) * (dp - delta)).astype(BF16)
                dv_acc[krows(j), :] += dot(p, do, NN)
                dk_acc[krows(j), :] += dot(ds, q, NN)
                oq_scr[...] += dot(kt[:, krows(j)], ds, NN)
                return carry

            lax.fori_loop(0, full + per, back, 0)
            out_ref[1, qrows, :] = (oq_scr[...] * c).astype(BF16).T
            return carry

        lax.fori_loop(0, nqb, q_block, 0)

        def finish(i, carry):
            rows = pl.ds(pl.multiple_of(i * kb, kb), kb)
            out_ref[2, rows, :] = (dk_acc[rows, :] * c).astype(BF16)
            out_ref[3, rows, :] = dv_acc[rows, :].astype(BF16)
            return carry

        lax.fori_loop(0, seq // kb, finish, 0)


def solution(mesh):
    devs = mesh.shape["cp"]

    def attend_layer(x_loc, dy_loc, w_q, w_k, w_v, w_o):
        tok = x_loc.shape[0]
        half = tok // 2
        heads, e = w_q.shape[1:]
        seq = devs * tok
        qb = min(QB, seq)
        kb = min(KB, seq)

        def project(weight):
            return jnp.einsum("td,dhe->hte", x_loc, weight, preferred_element_type=F32).astype(BF16)

        d_out = jnp.einsum("td,hed->hte", dy_loc, w_o, preferred_element_type=F32).astype(BF16)
        packed = jnp.stack([project(w_q), project(w_k), project(w_v), d_out], axis=1)
        packed = packed.reshape(heads, 4, 2, half, e)
        hbm = pl.BlockSpec(memory_space=pl.ANY)
        sems = [pltpu.SemaphoreType.DMA, pltpu.SemaphoreType.DMA]
        by_head = pl.pallas_call(
            functools.partial(gather_kernel, heads, devs),
            out_shape=jax.ShapeDtypeStruct((4, 2 * devs, half, e), BF16),
            in_specs=[hbm], out_specs=hbm, scratch_shapes=sems, name="rows_to_heads",
            compiler_params=pltpu.CompilerParams(has_side_effects=True))(packed)
        vmem = pl.BlockSpec(memory_space=pltpu.VMEM)
        grads = pl.pallas_call(
            functools.partial(attend_kernel, heads, devs, qb, kb),
            out_shape=jax.ShapeDtypeStruct((4, seq, e), BF16),
            in_specs=[vmem], out_specs=vmem, name="attend",
            scratch_shapes=[
                pltpu.VMEM((e, seq), BF16), pltpu.VMEM((e, seq), BF16), pltpu.VMEM((e, seq), BF16),
                pltpu.VMEM((seq, qb), F32), pltpu.VMEM((seq, qb), BF16),
                pltpu.VMEM((seq, e), F32), pltpu.VMEM((seq, e), F32), pltpu.VMEM((e, qb), F32)],
            compiler_params=pltpu.CompilerParams(vmem_limit_bytes=48 << 20))(by_head.reshape(4, seq, e))
        back = pl.pallas_call(
            functools.partial(scatter_kernel, heads, devs),
            out_shape=jax.ShapeDtypeStruct((heads, 4, 2, half, e), BF16),
            in_specs=[hbm], out_specs=hbm, scratch_shapes=sems, name="heads_to_rows",
            compiler_params=pltpu.CompilerParams(has_side_effects=True))(grads.reshape(4, 2 * devs, half, e))
        back = back.reshape(heads, 4, tok, e)
        y_loc = jnp.einsum("hte,hed->td", back[:, 0], w_o, preferred_element_type=F32).astype(BF16)
        dx = (jnp.einsum("hte,dhe->td", back[:, 1], w_q, preferred_element_type=F32)
              + jnp.einsum("hte,dhe->td", back[:, 2], w_k, preferred_element_type=F32)
              + jnp.einsum("hte,dhe->td", back[:, 3], w_v, preferred_element_type=F32))
        return y_loc, dx.astype(BF16)

    row_spec = P(("dp", "cp"), None)
    full_spec = P(None, None, None)
    return jax.shard_map(
        attend_layer, mesh=mesh,
        in_specs=(row_spec, row_spec, full_spec, full_spec, full_spec, full_spec),
        out_specs=(row_spec, row_spec), check_vma=False)
```
